32 devices in a mesh: groups: 2 (over y), seq: 8 (over z, x), tp: 2 (over core).
Axes of the slice: x: 2, y: 2, z: 4, core: 2. Of those that a mesh axis runs over, the one named last changes fastest.
Arguments:
- stream: bfloat16 [128, 6144], P(('groups', 'seq'), 'tp'), parts along dimension 0, may hold values from -6 to 6
- queries: bfloat16 [128, 6144], P(('groups', 'seq'), 'tp'), parts along dimension 0, may hold values from -6 to 6
- key_rows: bfloat16 [128, 1024], P(('groups', 'seq'), 'tp'), parts along dimension 0, may hold values from -6 to 6
- value_rows: bfloat16 [128, 1024], P(('groups', 'seq'), 'tp'), parts along dimension 0, may hold values from -6 to 6
- routes: int32 [128, 2], P(('groups', 'seq')), parts along dimension 0, may hold values from 0 to 3, all different within a row; in each aligned block of 8 rows (0 to 7, 8 to 15, ...) at most 4 rows name the same one
- seq_length: int32 [2], P('groups'), parts along dimension 0, may hold values from 16 to 64
- norm_gain: float32 [6144], P('tp'), may hold values from 0.25 to 1.75
- router: float32 [6144, 4], P('tp'), may hold values from -0.078125 to 0.078125
- w_up: bfloat16 [6144, 32768], P('tp', 'seq'), may hold values from -0.078125 to 0.078125
- w_down: bfloat16 [32768, 6144], P('seq', 'tp'), may hold values from -0.0625 to 0.0625
- final_gain: float32 [6144], P('tp'), may hold values from 0.25 to 1.75
- value_weight: float32 [6144], P('tp'), may hold values from -0.078125 to 0.078125
- value_bias: float32 [1], replicated, may hold values from -3 to 3
Outputs:
- layer_out: bfloat16 [128, 6144], P(('groups', 'seq'), 'tp'), parts along dimension 0
- values: float32 [128], P(('groups', 'seq')), parts along dimension 0
The draws below stay inside these ranges and needn't reach their ends.
There are 2 independent parts, one for each index of `groups`. The reference program is written for one: setup_inputs(seed, part) draws one part's arguments, and reference() takes and returns one part's arrays. A program takes and returns all parts, laid end to end along the dimension named above; an argument that names none is the same for every part. Nothing has to cross between parts.
Inputs may be any that keep to these rules, and one draw needn't show every extreme that they name: `routes`: each row names two different experts; among the rows on one device no expert is named more than 4 times, and some device's rows name some expert exactly 4 times.
All inputs are finite; a program needn't handle non-finite values.
Results may differ from the reference program's by a relative error of at most 0.01.
Values may be sent and summed in bfloat16 or wider, within the bound.
No kernel may reach another device: no remote copies, remote signals or barrier semaphores. Data moves between devices by JAX's collectives and lax.ppermute only.
A program may use at most 128 MiB of HBM per device.

```python
import math
import jax
import jax.numpy as jnp
import numpy as np
from jax import lax

D = 6144
HQ = 48
KVH = 8
HD = 128
EXPERTS = 4
F = 8192
LEN_DEV = 8
LENGTH = 64
CAP = 4
N_SEQ = 8


def draw_queries(key, part):
    values = jnp.clip(1.5 * jax.random.normal(jax.random.fold_in(key, 11), (LENGTH, HQ * HD), jnp.float32), -6.0, 6.0)
    return values.astype(jnp.bfloat16)


def draw_key_rows(key, part):
    values = jnp.clip(jax.random.normal(jax.random.fold_in(key, 12), (LENGTH, KVH * HD), jnp.float32), -6.0, 6.0)
    return values.astype(jnp.bfloat16)


def block_scale(stream_key, shape, split, least, top_value):
    gain = 1.0
    for position, shards_of in split:
        heights = jax.random.uniform(jax.random.fold_in(jax.random.fold_in(stream_key, 6), position), (shards_of,), jnp.float32, least / len(split), top_value / len(split))
        gain = gain * jnp.repeat(jnp.exp(heights), shape[position] // shards_of).reshape((-1,) + (1,) * (len(shape) - 1 - position))
    return gain


def shared_out(rng, own, number, rows, count, top, reach, lean):
    sequence = jax.random.permutation(rng, count)
    heavy_load, ordinary = shares(count, rows * top, reach, lean, True), shares(count, rows * top, reach, lean, False)
    places = jnp.arange(count)

    def named(lengths, rotation):
        used = int((lengths > 0).sum())
        fixed = max(1, used // 4)
        passed = fixed + (places - fixed + rotation * (used - fixed)) % max(1, count - fixed)
        return jnp.zeros((count,), jnp.int32).at[sequence[jnp.where(places < fixed, places, passed)]].set(jnp.asarray(lengths, jnp.int32))

    lengths = jnp.where(number % 4 == 0, named(heavy_load, number // 4), named(ordinary, number - number // 4 - 1))
    mixed = jax.random.permutation(jax.random.fold_in(own, 3), count)
    giver, taker = mixed[0:count // 2 * 2:2], mixed[1:count // 2 * 2:2]
    slack = jnp.minimum(lengths[giver] - 1, reach - lengths[taker]) // 2
    slack = jnp.where((giver == sequence[0]) | (taker == sequence[0]) | (lengths[taker] == 0), 0, jnp.maximum(slack, 0))
    passed = jax.random.randint(jax.random.fold_in(own, 4), (count // 2,), 0, 1 << 20) % (slack + 1)
    lengths = lengths.at[giver].add(-passed).at[taker].add(passed)
    members = jnp.searchsorted(jnp.cumsum(lengths), jnp.arange(rows * top), side="right").astype(jnp.int32)
    grid = members.reshape(top, rows).T
    grid = grid[jax.random.permutation(jax.random.fold_in(own, 1), rows)]
    rotation = jax.random.randint(jax.random.fold_in(own, 2), (rows, 1), 0, top)
    return jnp.take_along_axis(grid, (jnp.arange(top)[None, :] + rotation) % top, axis=1)


def shares(count, total, most, lean, full):
    portions = [(1 << 20) // math.isqrt(grade ** lean) + 1 for grade in range(1, count + 1)]
    largest = most if full else min(most, max(-(-total // count), total * portions[0] // sum(portions)))
    least = 1 if total - largest >= count - 1 else 0
    counts, spare = [largest] + [least] * (count - 1), total - largest - least * (count - 1)
    while spare > 0:
        movable = [i for i in range(1, count) if counts[i] < largest] or [i for i in range(1, count) if counts[i] < most]
        mass, remaining = sum([portions[i] for i in movable]), spare
        for i in movable:
            addition = min(most - counts[i], max(1, remaining * portions[i] // mass), spare)
            counts[i] = counts[i] + addition
            spare = spare - addition
    return np.array(counts)


def noise(own_key, extent, width, most, shards=(), kind=jnp.bfloat16):
    drawn = width * jax.random.normal(own_key, extent, jnp.float32)
    if shards:
        drawn = drawn * block_scale(own_key, extent, shards, -0.22, 0.18)
    return jnp.clip(drawn, -most, most).astype(kind)


def setup_inputs(seed: int = 0, part: int = 0) -> dict:
    arg_keys = jax.random.split(jax.random.key(seed), 14)
    part_keys = jax.random.split(jax.random.fold_in(arg_keys[13], part), 14)
    stream = noise(part_keys[0], (LENGTH, D), 1.0, 6.0, ((0, 8), (1, 2)))
    queries = draw_queries(jax.random.fold_in(jax.random.fold_in(arg_keys[13], part), 71), part)
    key_rows = draw_key_rows(jax.random.fold_in(jax.random.fold_in(arg_keys[13], part), 71), part)
    value_rows = noise(part_keys[3], (LENGTH, KVH * HD), 1.0, 6.0, ((0, 8), (1, 2)))
    routes_keys = jax.random.split(jax.random.fold_in(part_keys[4], 1), LENGTH // LEN_DEV)
    routes_turns = jax.random.permutation(jax.random.fold_in(part_keys[4], 3), LENGTH // LEN_DEV)
    routes = jax.vmap(lambda own, number: shared_out(jax.random.fold_in(part_keys[4], 2), own, number, LEN_DEV, EXPERTS, 2, CAP, 2))(routes_keys, routes_turns).reshape((LENGTH, 2))
    seq_length = jax.random.randint(part_keys[5], (1,), LENGTH // 4, LENGTH + 1).astype(jnp.int32)
    norm_gain = jnp.clip(1.0 + 0.15 * jax.random.normal(arg_keys[6], (D,), jnp.float32), 0.25, 1.75)
    router = noise(arg_keys[7], (D, EXPERTS), D ** -0.5, 0.078125, ((0, 2),), jnp.float32)
    w_up = noise(arg_keys[8], (D, EXPERTS * F), D ** -0.5, 0.078125, ((0, 2), (1, 8)))
    w_down = noise(arg_keys[9], (EXPERTS * F, D), F ** -0.5, 0.0625, ((0, 8), (1, 2)))
    final_gain = jnp.clip(1.0 + 0.15 * jax.random.normal(arg_keys[10], (D,), jnp.float32), 0.25, 1.75)
    value_weight = noise(arg_keys[11], (D,), D ** -0.5, 0.078125, ((0, 2),), jnp.float32)
    value_bias = noise(arg_keys[12], (1,), 1.0, 3.0, (), jnp.float32)
    return dict(stream=stream, queries=queries, key_rows=key_rows, value_rows=value_rows, routes=routes, seq_length=seq_length, norm_gain=norm_gain, router=router, w_up=w_up, w_down=w_down, final_gain=final_gain, value_weight=value_weight, value_bias=value_bias)


eps = 1e-05

def attention(queries, key_rows, value_rows, seq_limit):
    per_group = HQ // KVH
    positions = jnp.arange(LENGTH, dtype=jnp.int32)
    allowed = (positions[None, :] <= positions[:, None]) & (positions[None, :] < seq_limit)
    q_heads = queries.reshape(LENGTH, KVH, per_group, HD).transpose(1, 2, 0, 3)
    k_heads = key_rows.reshape(LENGTH, KVH, HD).transpose(1, 0, 2)
    v_heads = value_rows.reshape(LENGTH, KVH, HD).transpose(1, 0, 2)

    def one_head(triple):
        q_one, k_one, v_one = triple
        scores = jnp.einsum('gqd,cd->gqc', q_one.astype(jnp.float32), k_one.astype(jnp.float32)) / math.sqrt(HD)
        scores = jnp.where(allowed, scores, -jnp.inf)
        top_score = lax.optimization_barrier(jnp.max(scores, axis=-1, keepdims=True))
        expo = jnp.where(allowed, jnp.exp(scores - top_score), 0.0)
        rounded = lax.optimization_barrier(expo.astype(jnp.bfloat16))
        numer = jnp.einsum('gqc,cd->gqd', rounded.astype(jnp.float32), v_one.astype(jnp.float32))
        return numer / lax.optimization_barrier(jnp.sum(expo, axis=-1))[..., None]
    heads = lax.map(one_head, (q_heads, k_heads, v_heads))
    return heads.transpose(2, 0, 1, 3).reshape(LENGTH, HQ * HD)

def reference(stream, queries, key_rows, value_rows, routes, seq_length, norm_gain, router, w_up, w_down, final_gain, value_weight, value_bias):
    seq_limit = seq_length[0]
    hidden = stream.astype(jnp.float32) + attention(queries, key_rows, value_rows, seq_limit)
    normed = hidden * lax.rsqrt(lax.optimization_barrier(jnp.mean(hidden * hidden, axis=1, keepdims=True)) + eps) * norm_gain
    normed_half = normed.astype(jnp.bfloat16)
    logits = jnp.dot(normed, router, precision=lax.Precision.HIGHEST)
    chosen = (routes[:, :, None] == jnp.arange(EXPERTS, dtype=jnp.int32)).astype(jnp.float32)
    picked = lax.optimization_barrier(jnp.sum(chosen * logits[:, None, :], axis=2))
    gates = jax.nn.sigmoid(picked - picked[:, ::-1])
    coeffs = lax.optimization_barrier(jnp.sum(chosen * gates[:, :, None], axis=1))
    owners = N_SEQ // EXPERTS
    block = F // owners
    mixed = jnp.zeros((LENGTH, D), jnp.float32)
    for expert in range(EXPERTS):
        up_proj = jnp.dot(normed_half, w_up[:, expert * F:(expert + 1) * F], preferred_element_type=jnp.float32)
        active = jax.nn.silu(up_proj).astype(jnp.bfloat16)
        down_rows = w_down[expert * F:(expert + 1) * F]

        def add_block(total, index):
            act_part = lax.dynamic_slice_in_dim(active, index * block, block, 1)
            weight_part = lax.dynamic_slice_in_dim(down_rows, index * block, block, 0)
            piece = jnp.dot(act_part, weight_part, preferred_element_type=jnp.float32).astype(jnp.bfloat16)
            return (total + lax.optimization_barrier(piece).astype(jnp.float32), None)
        expert_out, _ = lax.scan(add_block, jnp.zeros((LENGTH, D), jnp.float32), jnp.arange(owners, dtype=jnp.int32))
        mixed = mixed + coeffs[:, expert:expert + 1] * expert_out
    final = hidden + mixed
    mean_sq = lax.optimization_barrier(jnp.mean(final * final, axis=1))
    estimate = lax.optimization_barrier(jnp.sum(final * final_gain * value_weight, axis=1)) * lax.rsqrt(mean_sq + eps) + value_bias[0]
    positions = jnp.arange(LENGTH, dtype=jnp.int32)
    estimate = jnp.where(positions < seq_limit, estimate, 0.0)
    return (final.astype(jnp.bfloat16), estimate)
```

```python
import math

import jax
import jax.numpy as jnp
from jax import lax
from jax.experimental import pallas as pl
from jax.experimental.pallas import tpu as pltpu
from jax.sharding import PartitionSpec as P

D = 6144
HD = 128
EXPERTS = 4


eps = 1e-05
masked = -1e30


bf16 = jnp.bfloat16
f32 = jnp.float32
VMEM_REF = pl.BlockSpec(memory_space=pltpu.VMEM)
SMEM_REF = pl.BlockSpec(memory_space=pltpu.SMEM)


def iota(shape, dim):
    return lax.broadcasted_iota(jnp.int32, shape, dim)


def struct(shape, dtype):
    return jax.ShapeDtypeStruct(shape, dtype)


def kernel(name, body, outs, *args, smem=(), flops=10**6, limit=8, scratch=()):
    return pl.pallas_call(
        body,
        out_shape=outs,
        in_specs=[SMEM_REF if i in smem else VMEM_REF for i in range(len(args))],
        out_specs=jax.tree.map(lambda _: VMEM_REF, outs),
        scratch_shapes=list(scratch),
        compiler_params=pltpu.CompilerParams(vmem_limit_bytes=limit << 20),
        cost_estimate=pl.CostEstimate(flops=flops, bytes_accessed=10**5, transcendentals=0),
        name=name,
    )(*args)


def hits(routes_t, group, cap, reps):
    count = EXPERTS * reps * cap
    tokens = routes_t.shape[1]
    row = iota((count, tokens), 0)
    expert = group ^ (row // (reps * cap))
    first = routes_t[0:1, :] == expert
    second = routes_t[1:2, :] == expert
    hit = jnp.where(first | second, 1.0, 0.0).astype(f32)
    earlier = jnp.where(iota((tokens, tokens), 0) < iota((tokens, tokens), 1), 1.0, 0.0).astype(f32)
    rank = jnp.dot(hit, earlier, preferred_element_type=f32)
    mine = jnp.where(rank == (row % cap).astype(f32), hit, 0.0)
    return row, first, mine


def attend(q_rows, keys, vals, allowed, per_group):
    rows = q_rows.shape[0]
    stacked = jnp.concatenate([q_rows[:, h * HD : (h + 1) * HD] for h in range(per_group)], 0)
    scores = lax.dot_general(
        stacked.astype(bf16), keys, (((1,), (1,)), ((), ())), preferred_element_type=f32
    ) * (1.0 / math.sqrt(HD))
    mask = jnp.concatenate([allowed] * per_group, 0) > 0.5
    scores = jnp.where(mask, scores, masked)
    top = jnp.max(scores, axis=1, keepdims=True)
    expo = jnp.where(mask, jnp.exp(scores - top), 0.0)
    total = jnp.sum(expo, axis=1, keepdims=True)
    out = jnp.dot(expo.astype(bf16), vals, preferred_element_type=f32) / total
    return jnp.concatenate([out[h * rows : (h + 1) * rows] for h in range(per_group)], 1)


def on_device(
    stream,
    queries,
    key_rows,
    value_rows,
    routes,
    seq_length,
    norm_gain,
    router,
    w_up,
    w_down,
    final_gain,
    value_weight,
    value_bias,
):
    tokens, half = stream.shape
    kv_width = key_rows.shape[1]
    kv_heads = kv_width // HD
    per_group = half // HD // kv_heads
    hidden_units = w_up.shape[1]
    devices = lax.axis_size("seq")
    owners = devices // EXPERTS
    cap = tokens // 2
    width = half * lax.axis_size("tp")
    k_at, v_at, meta_at = half, half + kv_width, half + 2 * kv_width
    cols = meta_at + HD
    rows = devices * cap
    order = [j * owners + x for x in range(owners) for j in range(EXPERTS)]
    routes_t = routes.T
    swap = [(0, 1), (1, 0)]

    def pack(stream_ref, q_ref, k_ref, v_ref, routes_ref, *outs):
        group = lax.axis_index("seq") // owners
        row, _, mine = hits(routes_ref[...], group, cap, 2)
        upper = (row // cap) % 2 == 0
        q_pick = jnp.where(upper, mine, 0.0).astype(bf16)
        s_pick = jnp.where(upper, 0.0, mine).astype(bf16)
        picked = jnp.dot(q_pick, q_ref[...], preferred_element_type=f32) + jnp.dot(
            s_pick, stream_ref[...], preferred_element_type=f32
        )
        place = jnp.sum(mine * iota(mine.shape, 1).astype(f32), axis=1, keepdims=True)
        place = jnp.broadcast_to(place, (mine.shape[0], HD))
        for j, out in enumerate(outs):
            out[:, 0:half] = picked[j * tokens : (j + 1) * tokens].astype(bf16)
            out[:, k_at:v_at] = k_ref[...]
            out[:, v_at:meta_at] = v_ref[...]
            out[:, meta_at:cols] = place[j * tokens : (j + 1) * tokens].astype(bf16)

    payloads = kernel(
        "pack",
        pack,
        [struct((tokens, cols), bf16)] * EXPERTS,
        stream,
        queries,
        key_rows,
        value_rows,
        routes_t,
        flops=10**11,
    )
    parcels = [
        payloads[0] if s == 0 else lax.ppermute(payloads[s // owners], "seq", [(i, i ^ s) for i in range(devices)])
        for s in range(devices)
    ]

    def keys_of(parcel_refs, at):
        return jnp.concatenate([p[:, at : at + kv_width].astype(f32) for p in parcel_refs], 0).astype(bf16)

    def key_places(shape, me):
        key = iota(shape, 1)
        return (me ^ (key // tokens)) * tokens + key % tokens

    def up(*refs):
        parcel_refs = refs[:devices]
        limit_ref, gain_ref, w_ref, own_ref, send_ref, sq_ref, x_ref = refs[devices:]
        me = lax.axis_index("seq")
        keys = keys_of(parcel_refs, k_at)
        vals = keys_of(parcel_refs, v_at)
        upper = [parcel_refs[s][:, 0:half].astype(f32) for s in order]
        q_rows = jnp.concatenate([u[0:cap] for u in upper], 0)
        base = jnp.concatenate([u[cap : 2 * cap] for u in upper], 0)
        meta = jnp.concatenate([parcel_refs[s][:, meta_at:cols].astype(f32)[0:cap] for s in order], 0)
        row = iota((rows, 1), 0)
        slot = row // cap
        source = me ^ ((slot % EXPERTS) * owners + slot // EXPERTS)
        place = source * tokens + meta[:, 0:1].astype(jnp.int32)
        key_at = key_places((rows, devices * tokens), me)
        allowed = jnp.where((key_at <= place) & (key_at < limit_ref[0]), 1.0, 0.0)
        gain = gain_ref[...].reshape(1, half)
        total = jnp.zeros((rows, 1), f32)
        span = per_group * HD
        for g in range(kv_heads):
            at = slice(g * span, (g + 1) * span)
            att = attend(
                q_rows[:, at], keys[:, g * HD : (g + 1) * HD], vals[:, g * HD : (g + 1) * HD], allowed, per_group
            )
            hidden = base[:, at] + att
            total = total + jnp.sum(hidden * hidden, axis=1, keepdims=True)
            x_ref[:, at] = (hidden * gain[:, at]).astype(bf16)
        part = jnp.dot(x_ref[...], w_ref[...], preferred_element_type=f32)
        own_ref[...] = part
        send_ref[:, 0:hidden_units] = part.astype(bf16)
        high = total.astype(bf16)
        low = (total - high.astype(f32)).astype(bf16)
        lane = iota((rows, HD), 1)
        send_ref[:, hidden_units:] = jnp.where(lane == 0, high.astype(f32), low.astype(f32)).astype(bf16)
        sq_ref[...] = jnp.broadcast_to(total, (rows, HD))

    own, send, own_sq = kernel(
        "up",
        up,
        [struct((rows, hidden_units), f32), struct((rows, hidden_units + HD), bf16), struct((rows, HD), f32)],
        *parcels,
        seq_length,
        norm_gain,
        w_up,
        smem=(devices,),
        scratch=(pltpu.VMEM((rows, half), bf16),),
        limit=8,
    )
    peer = lax.ppermute(send, "tp", swap)

    def home(*refs):
        parcel_refs = refs[:devices]
        limit_ref, stream_ref, q_ref, gain_ref, router_ref, hidden_ref, stat_ref = refs[devices:]
        me = lax.axis_index("seq")
        keys = keys_of(parcel_refs, k_at)
        vals = keys_of(parcel_refs, v_at)
        place = me * tokens + iota((tokens, 1), 0)
        key_at = key_places((tokens, devices * tokens), me)
        allowed = jnp.where((key_at <= place) & (key_at < limit_ref[0]), 1.0, 0.0)
        q_rows = q_ref[...].astype(f32)
        gain = gain_ref[...].reshape(1, half)
        total = jnp.zeros((tokens, 1), f32)
        logits = [jnp.zeros((tokens, 1), f32) for _ in range(EXPERTS)]
        span = per_group * HD
        for g in range(kv_heads):
            at = slice(g * span, (g + 1) * span)
            att = attend(
                q_rows[:, at], keys[:, g * HD : (g + 1) * HD], vals[:, g * HD : (g + 1) * HD], allowed, per_group
            )
            hidden = stream_ref[:, at].astype(f32) + att
            hidden_ref[:, at] = hidden
            total = total + jnp.sum(hidden * hidden, axis=1, keepdims=True)
            gained = hidden * gain[:, at]
            for e in range(EXPERTS):
                logits[e] = logits[e] + jnp.sum(gained * router_ref[e : e + 1, at], axis=1, keepdims=True)
        lane = iota((tokens, HD), 1)
        stat = jnp.where(lane == 0, total, 0.0)
        for e in range(EXPERTS):
            stat = jnp.where(lane == e + 1, logits[e], stat)
        stat_ref[...] = stat

    hidden, stat = kernel(
        "home",
        home,
        [struct((tokens, half), f32), struct((tokens, HD), f32)],
        *parcels,
        seq_length,
        stream,
        queries,
        norm_gain,
        router.T,
        smem=(devices,),
    )
    peer_stat = lax.ppermute(stat, "tp", swap)

    def down(own_ref, peer_ref, sq_ref, w_ref, keep_ref, *pass_refs):
        marks = peer_ref[:, hidden_units : hidden_units + HD].astype(f32)
        total = sq_ref[:, 0:1] + marks[:, 0:1] + marks[:, 1:2]
        scale = lax.rsqrt(total / width + eps)
        up_sum = (own_ref[...] + peer_ref[:, 0:hidden_units].astype(f32)) * scale
        active = (up_sum / (1.0 + jnp.exp(-up_sum))).astype(bf16)
        out = jnp.dot(active, w_ref[...], preferred_element_type=f32)
        block = EXPERTS * cap
        keep_ref[...] = out[0:block]
        for x, ref in enumerate(pass_refs):
            ref[...] = out[(x + 1) * block : (x + 2) * block].astype(bf16)

    block = EXPERTS * cap
    keep, *passing = kernel(
        "down",
        down,
        [struct((block, half), f32)] + [struct((block, half), bf16)] * (owners - 1),
        own,
        peer,
        own_sq,
        w_down,
    )
    passed = [
        lax.ppermute(passing[x - 1], "seq", [(i, i ^ x) for i in range(devices)]) for x in range(1, owners)
    ]

    def gather(keep_ref, *refs):
        total = keep_ref[...]
        for ref in refs[: owners - 1]:
            total = total + ref[...].astype(f32)
        for j, ref in enumerate(refs[owners - 1 :]):
            ref[...] = total[j * cap : (j + 1) * cap].astype(bf16)

    shares = kernel("gather", gather, [struct((cap, half), bf16)] * EXPERTS, keep, *passed)
    returned = [
        shares[0]
        if j == 0
        else lax.ppermute(shares[j], "seq", [(i, i ^ (j * owners)) for i in range(devices)])
        for j in range(EXPERTS)
    ]

    def combine(*refs):
        share_refs = refs[:EXPERTS]
        hidden_ref, stat_ref, peer_ref, routes_ref, gain_ref, value_ref, out_ref, tail_ref = refs[EXPERTS:]
        group = lax.axis_index("seq") // owners
        routes_now = routes_ref[...]
        _, first, mine = hits(routes_now, group, cap, 1)
        shares_all = jnp.concatenate([r[...].astype(f32) for r in share_refs], 0).astype(bf16)
        dims = (((0,), (0,)), ((), ()))
        one = lax.dot_general(
            jnp.where(first, mine, 0.0).astype(bf16), shares_all, dims, preferred_element_type=f32
        )
        two = lax.dot_general(
            jnp.where(first, 0.0, mine).astype(bf16), shares_all, dims, preferred_element_type=f32
        )
        eye = jnp.where(iota((tokens, tokens), 0) == iota((tokens, tokens), 1), 1.0, 0.0).astype(f32)
        column = lax.dot_general(
            eye, routes_now.astype(f32), (((1,), (1,)), ((), ())), preferred_element_type=f32
        )
        stat_all = stat_ref[...] + peer_ref[...]
        scale = lax.rsqrt(stat_all[:, 0:1] / width + eps)
        lane = iota((tokens, HD), 1).astype(f32) - 1.0
        picked = [
            jnp.sum(jnp.where(lane == column[:, c : c + 1], stat_all, 0.0), axis=1, keepdims=True) * scale
            for c in range(2)
        ]
        gate = [1.0 / (1.0 + jnp.exp(picked[1 - c] - picked[c])) for c in range(2)]
        final = hidden_ref[...] + (one * gate[0] + two * gate[1])
        out_ref[...] = final.astype(bf16)
        weight = (gain_ref[...] * value_ref[...]).reshape(1, half)
        sq_part = jnp.sum(final * final, axis=1, keepdims=True)
        dot_part = jnp.sum(final * weight, axis=1, keepdims=True)
        lanes = iota((tokens, HD), 1)
        tail_ref[...] = jnp.where(lanes == 0, sq_part, jnp.where(lanes == 1, dot_part, 0.0))

    out, tail = kernel(
        "combine",
        combine,
        [struct((tokens, half), bf16), struct((tokens, HD), f32)],
        *returned,
        hidden,
        stat,
        peer_stat,
        routes_t,
        final_gain,
        value_weight,
    )
    sums = tail + lax.ppermute(tail, "tp", swap)
    estimate = sums[:, 1] * lax.rsqrt(sums[:, 0] / width + eps) + value_bias[0]
    positions = lax.axis_index("seq") * tokens + jnp.arange(tokens, dtype=jnp.int32)
    return (out, jnp.where(positions < seq_length[0], estimate, 0.0))


def on_device_wide(
    stream,
    queries,
    key_rows,
    value_rows,
    routes,
    seq_length,
    norm_gain,
    router,
    w_up,
    w_down,
    final_gain,
    value_weight,
    value_bias,
):
    row_count = stream.shape[0]
    half_width = stream.shape[1]
    seq_devices = lax.axis_size("seq")
    owners = seq_devices // EXPERTS
    my_index = lax.axis_index("seq")
    seq_limit = seq_length[0]
    positions = my_index * row_count + jnp.arange(row_count, dtype=jnp.int32)
    kv_heads = key_rows.shape[1] // HD
    per_group = queries.shape[1] // HD // kv_heads
    grouped = queries.reshape(row_count, kv_heads, per_group, HD)
    inv_root = 1.0 / math.sqrt(HD)
    slot_cap = row_count // 2
    run_max = jnp.full((kv_heads, per_group, row_count), masked, jnp.float32)
    key_block = lax.all_gather(key_rows, "seq", axis=0, tiled=True)
    value_block = lax.all_gather(value_rows, "seq", axis=0, tiled=True)
    key_count = key_block.shape[0]
    scores = (
        jnp.einsum(
            "qkgd,ckd->kgqc",
            grouped,
            key_block.reshape(key_count, kv_heads, HD),
            preferred_element_type=jnp.float32,
        )
        * inv_root
    )
    key_pos = jnp.arange(key_count, dtype=jnp.int32)
    allowed = (key_pos[None, :] <= positions[:, None]) & (key_pos[None, :] < seq_limit)
    scores = jnp.where(allowed, scores, masked)
    new_max = jnp.maximum(run_max, jnp.max(scores, axis=-1))
    weights = jnp.where(allowed, jnp.exp(scores - new_max[..., None]), 0.0)
    new_sum = jnp.sum(weights, axis=-1)
    update = jnp.einsum(
        "kgqc,ckd->kgqd",
        weights.astype(jnp.bfloat16),
        value_block.reshape(key_count, kv_heads, HD),
        preferred_element_type=jnp.float32,
    )
    attended = (update / new_sum[..., None]).transpose(2, 0, 1, 3).reshape(row_count, half_width)
    hidden = stream.astype(jnp.float32) + attended
    gained = hidden * norm_gain
    squares = jnp.sum(hidden * hidden, axis=1)
    total_sq = lax.psum(squares, "tp")
    norm_scale = lax.rsqrt(total_sq / D + eps)
    normed = gained * norm_scale[:, None]
    logits = lax.psum(jnp.dot(normed, router, precision=lax.Precision.HIGHEST), "tp")
    normed_half = normed.astype(jnp.bfloat16)
    expert_ids = jnp.arange(EXPERTS, dtype=jnp.int32)
    chosen = (routes[:, :, None] == expert_ids).astype(jnp.float32)
    picked = jnp.sum(chosen * logits[:, None, :], axis=2)
    gates = jax.nn.sigmoid(picked - picked[:, ::-1])
    flat_hits = chosen.reshape(row_count * 2, EXPERTS)
    earlier = jnp.cumsum(flat_hits, axis=0) - flat_hits
    slot_index = jnp.sum(earlier * flat_hits, axis=1).astype(jnp.int32)
    target = routes.reshape(row_count * 2) * slot_cap + slot_index
    placing = (target[:, None] == jnp.arange(EXPERTS * slot_cap, dtype=jnp.int32)[None, :]).astype(
        jnp.bfloat16
    )
    doubled = jnp.repeat(normed_half, 2, axis=0)
    packed = jnp.einsum("pe,pd->ed", placing, doubled, preferred_element_type=jnp.float32).astype(
        jnp.bfloat16
    )
    outgoing = jnp.broadcast_to(
        packed.reshape(EXPERTS, 1, slot_cap, half_width), (EXPERTS, owners, slot_cap, half_width)
    ).reshape(seq_devices, slot_cap, half_width)
    arrived = lax.all_to_all(outgoing, "seq", split_axis=0, concat_axis=0, tiled=True)
    lead = arrived.shape[0]
    items = arrived.shape[1]
    flat_rows = arrived.reshape(lead * items, half_width)
    up_part = jnp.dot(flat_rows, w_up, preferred_element_type=jnp.float32)
    up_total = lax.psum(up_part.astype(jnp.bfloat16), "tp").astype(jnp.float32)
    active = jax.nn.silu(up_total).astype(jnp.bfloat16)
    down_part = jnp.dot(active, w_down, preferred_element_type=jnp.float32).astype(jnp.bfloat16)
    partial_out = down_part.reshape(lead, items, half_width)
    returned = lax.all_to_all(partial_out, "seq", split_axis=0, concat_axis=0, tiled=True)
    summed = jnp.sum(
        returned.reshape(EXPERTS, owners, slot_cap, half_width), axis=1, dtype=jnp.float32
    ).reshape(EXPERTS * slot_cap, half_width)
    fetched = jnp.dot(placing.astype(jnp.float32), summed, precision=lax.Precision.HIGHEST)
    mixed = jnp.sum(fetched.reshape(row_count, 2, half_width) * gates[:, :, None], axis=1)
    final = hidden + mixed
    sq_part = jnp.sum(final * final, axis=1)
    dot_part = jnp.sum(final * (final_gain * value_weight), axis=1)
    sq_total, dot_total = lax.psum((sq_part, dot_part), "tp")
    estimate = dot_total * lax.rsqrt(sq_total / D + eps) + value_bias[0]
    estimate = jnp.where(positions < seq_limit, estimate, 0.0)
    return (final.astype(jnp.bfloat16), estimate)


def solution(mesh):
    seq_devices = mesh.shape["seq"]
    small = seq_devices % EXPERTS == 0 and seq_devices & (seq_devices - 1) == 0 and seq_devices <= 16
    device_program = on_device if small and mesh.shape["tp"] == 2 else on_device_wide
    return jax.shard_map(
        device_program,
        mesh=mesh,
        in_specs=(
            P(("groups", "seq"), "tp"),
            P(("groups", "seq"), "tp"),
            P(("groups", "seq"), "tp"),
            P(("groups", "seq"), "tp"),
            P(("groups", "seq"), None),
            P("groups"),
            P("tp"),
            P("tp", None),
            P("tp", "seq"),
            P("seq", "tp"),
            P("tp"),
            P("tp"),
            P(),
        ),
        out_specs=(P(("groups", "seq"), "tp"), P(("groups", "seq"))),
        check_vma=False,
    )
```

```python
import math

import jax
import jax.numpy as jnp
from jax import lax
from jax.experimental import pallas as pl
from jax.experimental.pallas import tpu as pltpu
from jax.sharding import PartitionSpec as P

D = 6144
HD = 128
EXPERTS = 4


eps = 1e-05
masked = -1e30


bf16 = jnp.bfloat16
f32 = jnp.float32
VMEM_REF = pl.BlockSpec(memory_space=pltpu.VMEM)
SMEM_REF = pl.BlockSpec(memory_space=pltpu.SMEM)
HBM_REF = pl.BlockSpec(memory_space=pltpu.HBM)


def iota(shape, dim):
    return lax.broadcasted_iota(jnp.int32, shape, dim)


def struct(shape, dtype):
    return jax.ShapeDtypeStruct(shape, dtype)


def kernel(name, body, outs, *args, hbm=(), smem=(), vmem=(), flops=10**6, limit=8, scratch=()):
    spaces = {**dict.fromkeys(hbm, pltpu.HBM), **dict.fromkeys(vmem, pltpu.VMEM)}
    args = [pltpu.with_memory_space_constraint(a, spaces[i]) if i in spaces else a for i, a in enumerate(args)]
    return pl.pallas_call(
        body,
        out_shape=outs,
        in_specs=[HBM_REF if i in hbm else SMEM_REF if i in smem else VMEM_REF for i in range(len(args))],
        out_specs=jax.tree.map(lambda _: VMEM_REF, outs),
        scratch_shapes=list(scratch),
        compiler_params=pltpu.CompilerParams(vmem_limit_bytes=limit << 20),
        cost_estimate=pl.CostEstimate(flops=flops, bytes_accessed=10**5, transcendentals=0),
        name=name,
    )(*args)


def hits(routes_t, group, cap, reps):
    count = EXPERTS * reps * cap
    tokens = routes_t.shape[1]
    row = iota((count, tokens), 0)
    expert = group ^ (row // (reps * cap))
    first = routes_t[0:1, :] == expert
    second = routes_t[1:2, :] == expert
    hit = jnp.where(first | second, 1.0, 0.0).astype(f32)
    earlier = jnp.where(iota((tokens, tokens), 0) < iota((tokens, tokens), 1), 1.0, 0.0).astype(f32)
    rank = jnp.dot(hit, earlier, preferred_element_type=f32)
    mine = jnp.where(rank == (row % cap).astype(f32), hit, 0.0)
    return row, first, mine


def attend(q_rows, keys, vals, allowed, per_group):
    rows = q_rows.shape[0]
    stacked = jnp.concatenate([q_rows[:, h * HD : (h + 1) * HD] for h in range(per_group)], 0)
    scores = lax.dot_general(
        stacked.astype(bf16), keys, (((1,), (1,)), ((), ())), preferred_element_type=f32
    ) * (1.0 / math.sqrt(HD))
    mask = jnp.concatenate([allowed] * per_group, 0) > 0.5
    scores = jnp.where(mask, scores, masked)
    top = jnp.max(scores, axis=1, keepdims=True)
    expo = jnp.where(mask, jnp.exp(scores - top), 0.0)
    total = jnp.sum(expo, axis=1, keepdims=True)
    out = jnp.dot(expo.astype(bf16), vals, preferred_element_type=f32) / total
    return jnp.concatenate([out[h * rows : (h + 1) * rows] for h in range(per_group)], 1)


def on_device(
    stream,
    queries,
    key_rows,
    value_rows,
    routes,
    seq_length,
    norm_gain,
    router,
    w_up,
    w_down,
    final_gain,
    value_weight,
    value_bias,
):
    tokens, half = stream.shape
    kv_width = key_rows.shape[1]
    kv_heads = kv_width // HD
    per_group = half // HD // kv_heads
    hidden_units = w_up.shape[1]
    devices = lax.axis_size("seq")
    owners = devices // EXPERTS
    cap = tokens // 2
    width = half * lax.axis_size("tp")
    k_at, v_at, meta_at = half, half + kv_width, half + 2 * kv_width
    cols = meta_at + HD
    rows = devices * cap
    order = [j * owners + x for x in range(owners) for j in range(EXPERTS)]
    routes_t = routes.T
    swap = [(0, 1), (1, 0)]

    def pack(stream_hbm, q_hbm, k_hbm, v_hbm, routes_hbm, limit_ref, *refs):
        outs = refs[:EXPERTS]
        fixed_ref, stream_ref, q_ref, routes_ref, sems = refs[EXPERTS:]
        reads = [
            pltpu.make_async_copy(source, target, sems.at[n])
            for n, (source, target) in enumerate(
                [(routes_hbm, routes_ref), (q_hbm, q_ref), (stream_hbm, stream_ref)]
                + [(k_hbm, out.at[:, k_at:v_at]) for out in outs]
                + [(v_hbm, out.at[:, v_at:meta_at]) for out in outs]
            )
        ]
        for read in reads:
            read.start()
        reads[0].wait()
        group = lax.axis_index("seq") // owners
        row, _, mine = hits(routes_ref[...], group, cap, 2)
        upper = (row // cap) % 2 == 0
        q_pick = jnp.where(upper, mine, 0.0).astype(bf16)
        reads[1].wait()
        reads[2].wait()
        s_pick = jnp.where(upper, 0.0, mine).astype(bf16)
        picked = jnp.dot(q_pick, q_ref[...], preferred_element_type=f32) + jnp.dot(
            s_pick, stream_ref[...], preferred_element_type=f32
        )
        place = jnp.sum(mine * iota(mine.shape, 1).astype(f32), axis=1, keepdims=True)
        place = jnp.broadcast_to(place, (mine.shape[0], HD))
        for j, out in enumerate(outs):
            out[:, 0:half] = picked[j * tokens : (j + 1) * tokens].astype(bf16)
            out[:, meta_at:cols] = place[j * tokens : (j + 1) * tokens].astype(bf16)
        for read in reads[3:]:
            read.wait()
        fixed_ref[...] = jnp.full((tokens, HD), limit_ref[0], jnp.int32)

    *payloads, fixed = kernel(
        "pack",
        pack,
        [struct((tokens, cols), bf16)] * EXPERTS + [struct((tokens, HD), jnp.int32)],
        stream,
        queries,
        key_rows,
        value_rows,
        routes_t,
        seq_length,
        hbm=range(5),
        smem=(5,),
        scratch=(
            pltpu.VMEM((tokens, half), bf16),
            pltpu.VMEM((tokens, half), bf16),
            pltpu.VMEM((2, tokens), jnp.int32),
            pltpu.SemaphoreType.DMA((3 + 2 * EXPERTS,)),
        ),
        flops=10**11,
    )
    parcels = [
        payloads[0] if s == 0 else lax.ppermute(payloads[s // owners], "seq", [(i, i ^ s) for i in range(devices)])
        for s in range(devices)
    ]

    def keys_of(parcel_refs, at):
        return jnp.concatenate([p[:, at : at + kv_width].astype(f32) for p in parcel_refs], 0).astype(bf16)

    def key_places(shape, me):
        key = iota(shape, 1)
        return (me ^ (key // tokens)) * tokens + key % tokens

    def up(*refs):
        parcel_refs = refs[:devices]
        fixed_ref, gain_ref, w_ref, own_ref, send_ref, sq_ref, x_ref = refs[devices:]
        me = lax.axis_index("seq")
        keys = keys_of(parcel_refs, k_at)
        vals = keys_of(parcel_refs, v_at)
        upper = [parcel_refs[s][:, 0:half].astype(f32) for s in order]
        q_rows = jnp.concatenate([u[0:cap] for u in upper], 0)
        base = jnp.concatenate([u[cap : 2 * cap] for u in upper], 0)
        meta = jnp.concatenate([parcel_refs[s][:, meta_at:cols].astype(f32)[0:cap] for s in order], 0)
        row = iota((rows, 1), 0)
        slot = row // cap
        source = me ^ ((slot % EXPERTS) * owners + slot // EXPERTS)
        place = source * tokens + meta[:, 0:1].astype(jnp.int32)
        key_at = key_places((rows, devices * tokens), me)
        allowed = jnp.where((key_at <= place) & (key_at < fixed_ref[0:1, 0:1]), 1.0, 0.0)
        gain = gain_ref[...].reshape(1, half)
        total = jnp.zeros((rows, 1), f32)
        span = per_group * HD
        for g in range(kv_heads):
            at = slice(g * span, (g + 1) * span)
            att = attend(
                q_rows[:, at], keys[:, g * HD : (g + 1) * HD], vals[:, g * HD : (g + 1) * HD], allowed, per_group
            )
            hidden = base[:, at] + att
            total = total + jnp.sum(hidden * hidden, axis=1, keepdims=True)
            x_ref[:, at] = (hidden * gain[:, at]).astype(bf16)
        part = jnp.dot(x_ref[...], w_ref[...], preferred_element_type=f32)
        own_ref[...] = part
        send_ref[:, 0:hidden_units] = part.astype(bf16)
        high = total.astype(bf16)
        low = (total - high.astype(f32)).astype(bf16)
        lane = iota((rows, HD), 1)
        send_ref[:, hidden_units:] = jnp.where(lane == 0, high.astype(f32), low.astype(f32)).astype(bf16)
        sq_ref[...] = jnp.broadcast_to(total, (rows, HD))

    own, send, own_sq = kernel(
        "up",
        up,
        [struct((rows, hidden_units), f32), struct((rows, hidden_units + HD), bf16), struct((rows, HD), f32)],
        *parcels,
        fixed,
        norm_gain,
        w_up,
        vmem=(devices + 2,),
        scratch=(pltpu.VMEM((rows, half), bf16),),
    )
    peer = lax.ppermute(send, "tp", swap)

    def home(*refs):
        parcel_refs = refs[:devices]
        fixed_ref, stream_ref, q_ref, gain_ref, router_ref, hidden_ref, stat_ref = refs[devices:]
        me = lax.axis_index("seq")
        keys = keys_of(parcel_refs, k_at)
        vals = keys_of(parcel_refs, v_at)
        place = me * tokens + iota((tokens, 1), 0)
        key_at = key_places((tokens, devices * tokens), me)
        allowed = jnp.where((key_at <= place) & (key_at < fixed_ref[0:1, 0:1]), 1.0, 0.0)
        q_rows = q_ref[...].astype(f32)
        gain = gain_ref[...].reshape(1, half)
        total = jnp.zeros((tokens, 1), f32)
        logits = [jnp.zeros((tokens, 1), f32) for _ in range(EXPERTS)]
        span = per_group * HD
        for g in range(kv_heads):
            at = slice(g * span, (g + 1) * span)
            att = attend(
                q_rows[:, at], keys[:, g * HD : (g + 1) * HD], vals[:, g * HD : (g + 1) * HD], allowed, per_group
            )
            hidden = stream_ref[:, at].astype(f32) + att
            hidden_ref[:, at] = hidden
            total = total + jnp.sum(hidden * hidden, axis=1, keepdims=True)
            gained = hidden * gain[:, at]
            for e in range(EXPERTS):
                logits[e] = logits[e] + jnp.sum(gained * router_ref[e : e + 1, at], axis=1, keepdims=True)
        lane = iota((tokens, HD), 1)
        stat = jnp.where(lane == 0, total, 0.0)
        for e in range(EXPERTS):
            stat = jnp.where(lane == e + 1, logits[e], stat)
        stat_ref[...] = stat

    hidden, stat = kernel(
        "home",
        home,
        [struct((tokens, half), f32), struct((tokens, HD), f32)],
        *parcels,
        fixed,
        stream,
        queries,
        norm_gain,
        router.T,
    )
    peer_stat = lax.ppermute(stat, "tp", swap)

    def down(own_ref, peer_ref, sq_ref, w_ref, keep_ref, *pass_refs):
        marks = peer_ref[:, hidden_units : hidden_units + HD].astype(f32)
        total = sq_ref[:, 0:1] + marks[:, 0:1] + marks[:, 1:2]
        scale = lax.rsqrt(total / width + eps)
        up_sum = (own_ref[...] + peer_ref[:, 0:hidden_units].astype(f32)) * scale
        active = (up_sum / (1.0 + jnp.exp(-up_sum))).astype(bf16)
        out = jnp.dot(active, w_ref[...], preferred_element_type=f32)
        block = EXPERTS * cap
        keep_ref[...] = out[0:block]
        for x, ref in enumerate(pass_refs):
            ref[...] = out[(x + 1) * block : (x + 2) * block].astype(bf16)

    block = EXPERTS * cap
    keep, *passing = kernel(
        "down",
        down,
        [struct((block, half), f32)] + [struct((block, half), bf16)] * (owners - 1),
        own,
        peer,
        own_sq,
        w_down,
        vmem=(3,),
    )
    passed = [
        lax.ppermute(passing[x - 1], "seq", [(i, i ^ x) for i in range(devices)]) for x in range(1, owners)
    ]

    def gather(keep_ref, *refs):
        total = keep_ref[...]
        for ref in refs[: owners - 1]:
            total = total + ref[...].astype(f32)
        for j, ref in enumerate(refs[owners - 1 :]):
            ref[...] = total[j * cap : (j + 1) * cap].astype(bf16)

    shares = kernel("gather", gather, [struct((cap, half), bf16)] * EXPERTS, keep, *passed)
    returned = [
        shares[0]
        if j == 0
        else lax.ppermute(shares[j], "seq", [(i, i ^ (j * owners)) for i in range(devices)])
        for j in range(EXPERTS)
    ]

    def combine(*refs):
        share_refs = refs[:EXPERTS]
        hidden_ref, stat_ref, peer_ref, routes_ref, gain_ref, value_ref, out_ref, tail_ref = refs[EXPERTS:]
        group = lax.axis_index("seq") // owners
        routes_now = routes_ref[...]
        _, first, mine = hits(routes_now, group, cap, 1)
        shares_all = jnp.concatenate([r[...].astype(f32) for r in share_refs], 0).astype(bf16)
        dims = (((0,), (0,)), ((), ()))
        one = lax.dot_general(
            jnp.where(first, mine, 0.0).astype(bf16), shares_all, dims, preferred_element_type=f32
        )
        two = lax.dot_general(
            jnp.where(first, 0.0, mine).astype(bf16), shares_all, dims, preferred_element_type=f32
        )
        eye = jnp.where(iota((tokens, tokens), 0) == iota((tokens, tokens), 1), 1.0, 0.0).astype(f32)
        column = lax.dot_general(
            eye, routes_now.astype(f32), (((1,), (1,)), ((), ())), preferred_element_type=f32
        )
        stat_all = stat_ref[...] + peer_ref[...]
        scale = lax.rsqrt(stat_all[:, 0:1] / width + eps)
        lane = iota((tokens, HD), 1).astype(f32) - 1.0
        picked = [
            jnp.sum(jnp.where(lane == column[:, c : c + 1], stat_all, 0.0), axis=1, keepdims=True) * scale
            for c in range(2)
        ]
        gate = [1.0 / (1.0 + jnp.exp(picked[1 - c] - picked[c])) for c in range(2)]
        final = hidden_ref[...] + (one * gate[0] + two * gate[1])
        out_ref[...] = final.astype(bf16)
        weight = (gain_ref[...] * value_ref[...]).reshape(1, half)
        sq_part = jnp.sum(final * final, axis=1, keepdims=True)
        dot_part = jnp.sum(final * weight, axis=1, keepdims=True)
        lanes = iota((tokens, HD), 1)
        tail_ref[...] = jnp.where(lanes == 0, sq_part, jnp.where(lanes == 1, dot_part, 0.0))

    out, tail = kernel(
        "combine",
        combine,
        [struct((tokens, half), bf16), struct((tokens, HD), f32)],
        *returned,
        hidden,
        stat,
        peer_stat,
        routes_t,
        final_gain,
        value_weight,
    )
    peer_tail = lax.ppermute(tail, "tp", swap)

    def finish(tail_ref, peer_ref, fixed_ref, bias_ref, out_ref):
        sums = tail_ref[...] + peer_ref[...]
        estimate = sums[:, 1:2] * lax.rsqrt(sums[:, 0:1] / width + eps) + bias_ref[0]
        place = lax.axis_index("seq") * tokens + iota((tokens, 1), 0)
        estimate = jnp.where(place < fixed_ref[:, 0:1], estimate, 0.0)
        eye = iota((tokens, tokens), 0) == iota((tokens, tokens), 1)
        out_ref[...] = jnp.sum(jnp.where(eye, estimate, 0.0), axis=0, keepdims=True).reshape(tokens)

    values = kernel("finish", finish, struct((tokens,), f32), tail, peer_tail, fixed, value_bias, smem=(3,))
    return (out, values)


def on_device_wide(
    stream,
    queries,
    key_rows,
    value_rows,
    routes,
    seq_length,
    norm_gain,
    router,
    w_up,
    w_down,
    final_gain,
    value_weight,
    value_bias,
):
    row_count = stream.shape[0]
    half_width = stream.shape[1]
    seq_devices = lax.axis_size("seq")
    owners = seq_devices // EXPERTS
    my_index = lax.axis_index("seq")
    seq_limit = seq_length[0]
    positions = my_index * row_count + jnp.arange(row_count, dtype=jnp.int32)
    kv_heads = key_rows.shape[1] // HD
    per_group = queries.shape[1] // HD // kv_heads
    grouped = queries.reshape(row_count, kv_heads, per_group, HD)
    inv_root = 1.0 / math.sqrt(HD)
    slot_cap = row_count // 2
    run_max = jnp.full((kv_heads, per_group, row_count), masked, jnp.float32)
    key_block = lax.all_gather(key_rows, "seq", axis=0, tiled=True)
    value_block = lax.all_gather(value_rows, "seq", axis=0, tiled=True)
    key_count = key_block.shape[0]
    scores = (
        jnp.einsum(
            "qkgd,ckd->kgqc",
            grouped,
            key_block.reshape(key_count, kv_heads, HD),
            preferred_element_type=jnp.float32,
        )
        * inv_root
    )
    key_pos = jnp.arange(key_count, dtype=jnp.int32)
    allowed = (key_pos[None, :] <= positions[:, None]) & (key_pos[None, :] < seq_limit)
    scores = jnp.where(allowed, scores, masked)
    new_max = jnp.maximum(run_max, jnp.max(scores, axis=-1))
    weights = jnp.where(allowed, jnp.exp(scores - new_max[..., None]), 0.0)
    new_sum = jnp.sum(weights, axis=-1)
    update = jnp.einsum(
        "kgqc,ckd->kgqd",
        weights.astype(jnp.bfloat16),
        value_block.reshape(key_count, kv_heads, HD),
        preferred_element_type=jnp.float32,
    )
    attended = (update / new_sum[..., None]).transpose(2, 0, 1, 3).reshape(row_count, half_width)
    hidden = stream.astype(jnp.float32) + attended
    gained = hidden * norm_gain
    squares = jnp.sum(hidden * hidden, axis=1)
    total_sq = lax.psum(squares, "tp")
    norm_scale = lax.rsqrt(total_sq / D + eps)
    normed = gained * norm_scale[:, None]
    logits = lax.psum(jnp.dot(normed, router, precision=lax.Precision.HIGHEST), "tp")
    normed_half = normed.astype(jnp.bfloat16)
    expert_ids = jnp.arange(EXPERTS, dtype=jnp.int32)
    chosen = (routes[:, :, None] == expert_ids).astype(jnp.float32)
    picked = jnp.sum(chosen * logits[:, None, :], axis=2)
    gates = jax.nn.sigmoid(picked - picked[:, ::-1])
    flat_hits = chosen.reshape(row_count * 2, EXPERTS)
    earlier = jnp.cumsum(flat_hits, axis=0) - flat_hits
    slot_index = jnp.sum(earlier * flat_hits, axis=1).astype(jnp.int32)
    target = routes.reshape(row_count * 2) * slot_cap + slot_index
    placing = (target[:, None] == jnp.arange(EXPERTS * slot_cap, dtype=jnp.int32)[None, :]).astype(
        jnp.bfloat16
    )
    doubled = jnp.repeat(normed_half, 2, axis=0)
    packed = jnp.einsum("pe,pd->ed", placing, doubled, preferred_element_type=jnp.float32).astype(
        jnp.bfloat16
    )
    outgoing = jnp.broadcast_to(
        packed.reshape(EXPERTS, 1, slot_cap, half_width), (EXPERTS, owners, slot_cap, half_width)
    ).reshape(seq_devices, slot_cap, half_width)
    arrived = lax.all_to_all(outgoing, "seq", split_axis=0, concat_axis=0, tiled=True)
    lead = arrived.shape[0]
    items = arrived.shape[1]
    flat_rows = arrived.reshape(lead * items, half_width)
    up_part = jnp.dot(flat_rows, w_up, preferred_element_type=jnp.float32)
    up_total = lax.psum(up_part.astype(jnp.bfloat16), "tp").astype(jnp.float32)
    active = jax.nn.silu(up_total).astype(jnp.bfloat16)
    down_part = jnp.dot(active, w_down, preferred_element_type=jnp.float32).astype(jnp.bfloat16)
    partial_out = down_part.reshape(lead, items, half_width)
    returned = lax.all_to_all(partial_out, "seq", split_axis=0, concat_axis=0, tiled=True)
    summed = jnp.sum(
        returned.reshape(EXPERTS, owners, slot_cap, half_width), axis=1, dtype=jnp.float32
    ).reshape(EXPERTS * slot_cap, half_width)
    fetched = jnp.dot(placing.astype(jnp.float32), summed, precision=lax.Precision.HIGHEST)
    mixed = jnp.sum(fetched.reshape(row_count, 2, half_width) * gates[:, :, None], axis=1)
    final = hidden + mixed
    sq_part = jnp.sum(final * final, axis=1)
    dot_part = jnp.sum(final * (final_gain * value_weight), axis=1)
    sq_total, dot_total = lax.psum((sq_part, dot_part), "tp")
    estimate = dot_total * lax.rsqrt(sq_total / D + eps) + value_bias[0]
    estimate = jnp.where(positions < seq_limit, estimate, 0.0)
    return (final.astype(jnp.bfloat16), estimate)


def solution(mesh):
    seq_devices = mesh.shape["seq"]
    small = seq_devices % EXPERTS == 0 and seq_devices & (seq_devices - 1) == 0 and seq_devices <= 16
    device_program = on_device if small and mesh.shape["tp"] == 2 else on_device_wide
    return jax.shard_map(
        device_program,
        mesh=mesh,
        in_specs=(
            P(("groups", "seq"), "tp"),
            P(("groups", "seq"), "tp"),
            P(("groups", "seq"), "tp"),
            P(("groups", "seq"), "tp"),
            P(("groups", "seq"), None),
            P("groups"),
            P("tp"),
            P("tp", None),
            P("tp", "seq"),
            P("seq", "tp"),
            P("tp"),
            P("tp"),
            P(),
        ),
        out_specs=(P(("groups", "seq"), "tp"), P(("groups", "seq"))),
        check_vma=False,
    )
```
